32 devices in a mesh: grp: 2 (over x), tp: 8 (over z, y), tower: 2 (over core).
Axes of the slice: x: 2, y: 2, z: 4, core: 2. Of those that a mesh axis runs over, the one named last changes fastest.
Arguments:
- hidden: bfloat16 [2, 512, 3072], P('tower', ('grp', 'tp')), parts along dimension 1, may hold values from -6 to 6
- modulation: float32 [2, 3, 3072], P('tower'), may hold values from -3 to 7, as said below
- qk_gains: float32 [2, 3, 1024], P('tower', None, 'tp'), may hold values from 0.75 to 13
- counts: int32 [2, 2], P(None, 'grp'), parts along dimension 1, may hold values from 64 to 256
- offsets: int32 [2, 2], P(None, 'grp'), parts along dimension 1, may hold values from 0 to 8191
- in_weights: bfloat16 [2, 3072, 4, 1024], P('tower', None, None, 'tp'), may hold values from -0.109375 to 0.109375
- out_weights: bfloat16 [2, 2, 1024, 3072], P('tower', None, 'tp'), may hold values from -0.5 to 0.5
Outputs:
- updated: bfloat16 [2, 512, 3072], P('tower', ('grp', 'tp')), parts along dimension 1
The draws below stay inside these ranges and needn't reach their ends.
There are 2 independent parts, one for each index of `grp`. The reference program is written for one: setup_inputs(seed, part) draws one part's arguments, and reference() takes and returns one part's arrays. A program takes and returns all parts, laid end to end along the dimension named above; an argument that names none is the same for every part. Nothing has to cross between parts.
Inputs may be any that keep to these rules, and one draw needn't show every extreme that they name: `modulation`: rows are shift, scale and gate.
All inputs are finite; a program needn't handle non-finite values.
Results may differ from the reference program's by a relative error of at most 0.025.
The reference program's roundings to bfloat16 on the way (of `normed`, `projected`, `self_out` and `cross_out`) count: a program that leaves them out, or rounds other values in their place, can miss the bound.
Values may be sent and summed in bfloat16 or wider, within the bound.
A program may use at most 64 MiB of HBM per device.

```python
import math
import jax
import jax.numpy as jnp
from jax import lax

D = 3072
HD = 128
TOK = 256
HEADS = 8
HW = 1024
N_TP = 8


def draw_modulation(key, part):
    first_key, second_key, third_key = jax.random.split(key, 3)
    shift = jnp.clip(0.5 * jax.random.normal(first_key, (2, D), jnp.float32), -3.0, 3.0)
    scale = jnp.clip(0.3 * jax.random.normal(second_key, (2, D), jnp.float32), -0.9, 3.0)
    gate = jax.random.uniform(third_key, (2, D), jnp.float32, 0.5, 1.5)
    return jnp.stack([shift, scale, gate], 1).astype(jnp.float32)


def draw_qk_gains(key, part):
    order_key, placing_key, rough_key = jax.random.split(jax.random.fold_in(key, 17), 3)
    ranking = jax.random.permutation(order_key, HEADS).astype(jnp.float32)
    placing = (ranking + jax.random.uniform(placing_key, (HEADS,), jnp.float32)) / HEADS
    top_log = math.log(2.0)
    head_scale = jnp.exp(top_log * placing)
    roughness = jnp.exp(jax.random.uniform(rough_key, (2, 3, HEADS, HD), jnp.float32, -0.25, 0.25))
    return (head_scale[None, None, :, None] * roughness).reshape(2, 3, HW).astype(jnp.float32)


def level_of(own_key, extent, cuts, low, high):
    loudness, own = 1.0, jax.random.fold_in(own_key, 6)
    for dim, parts in cuts:
        draws = jnp.exp(jax.random.uniform(jax.random.fold_in(own, dim), (parts,), jnp.float32, low / len(cuts), high / len(cuts)))
        loudness = loudness * jnp.repeat(draws, extent[dim] // parts).reshape([-1 if axis == dim else 1 for axis in range(len(extent))])
    return loudness


def scatter_about(stream_key, dims, scale, most, shards=(), kind=jnp.bfloat16):
    entries = jax.random.normal(stream_key, dims, jnp.float32) * scale
    if len(shards) > 0:
        entries = level_of(stream_key, dims, shards, -0.22, 0.18) * entries
    return jnp.clip(entries, min=-most, max=most).astype(kind)


def setup_inputs(seed: int = 0, part: int = 0) -> dict:
    splits = jax.random.split(jax.random.key(seed), 8)
    own_keys = jax.random.split(jax.random.fold_in(splits[7], part), 8)
    hidden = scatter_about(own_keys[0], (2, TOK, D), 1.0, 6.0, ((0, 2), (1, 8)))
    modulation = draw_modulation(jax.random.fold_in(splits[7], 71), part)
    qk_gains = draw_qk_gains(jax.random.fold_in(splits[7], 71), part)
    counts = jax.random.randint(own_keys[3], (2, 1), TOK // 4, TOK + 1).astype(jnp.int32)
    offsets = jax.random.randint(own_keys[4], (2, 1), 0, 8192).astype(jnp.int32)
    in_weights = scatter_about(splits[5], (2, D, 4, HW), D ** -0.5, 0.109375, ((0, 2), (3, 8)))
    out_weights = scatter_about(splits[6], (2, 2, HW, D), HD ** -0.5, 0.5, ((0, 2), (2, 8)))
    return {"hidden": hidden, "modulation": modulation, "qk_gains": qk_gains, "counts": counts, "offsets": offsets, "in_weights": in_weights, "out_weights": out_weights}


epsilon = 1e-06
rope_base = 10000.0
masked_score = -1e+30

def layer_norm(states):
    centre = states - lax.optimization_barrier(jnp.mean(states, -1, keepdims=True))
    spread = lax.optimization_barrier(jnp.mean(centre * centre, -1, keepdims=True))
    return centre * lax.rsqrt(spread + epsilon)

def rotate(columns, positions):
    head_width = columns.shape[-1]
    pair_index = jnp.arange(head_width // 2, dtype=jnp.int32)
    frequency = jnp.exp(pair_index.astype(jnp.float32) * (-2.0 * math.log(rope_base) / head_width))
    angles = positions.reshape((positions.shape[0],) + (1,) * (columns.ndim - 1)) * frequency
    cosine = jnp.cos(angles)
    sine_table = jnp.sin(angles)
    even_part = columns[..., 0::2]
    odd_part = columns[..., 1::2]
    turned = jnp.stack([even_part * cosine - odd_part * sine_table, even_part * sine_table + odd_part * cosine], -1)
    return turned.reshape(columns.shape)

def finish(projected, head_gains, positions):
    query_like = jnp.stack([projected[:, 0], projected[:, 1], projected[:, 3]], 1)
    squares = lax.optimization_barrier(jnp.mean(query_like * query_like, -1, keepdims=True))
    query_like = query_like * lax.rsqrt(squares + epsilon) * head_gains[None]
    turned = rotate(query_like, positions)
    return jnp.stack([turned[:, 0], turned[:, 1], projected[:, 2], turned[:, 2]], 1)

def attend(queries, key_rows, value_rows, key_count):
    scores = jnp.dot(queries, key_rows.T, preferred_element_type=jnp.float32) * (1.0 / math.sqrt(queries.shape[-1]))
    usable = jnp.arange(key_rows.shape[0], dtype=jnp.int32) < key_count
    scores = jnp.where(usable[None, :], scores, masked_score)
    row_max = lax.optimization_barrier(jnp.max(scores, -1, keepdims=True))
    raised = jnp.exp(scores - row_max)
    attention = (raised / lax.optimization_barrier(jnp.sum(raised, -1, keepdims=True))).astype(jnp.bfloat16)
    return jnp.dot(attention, value_rows, preferred_element_type=jnp.float32).astype(jnp.bfloat16)

def prepare(tower_index, hidden, modulation, qk_gains, offsets, in_weights):
    states = hidden[tower_index].astype(jnp.float32)
    modulate = modulation[tower_index]
    normed = (layer_norm(states) * (1.0 + modulate[1]) + modulate[0]).astype(jnp.bfloat16)
    projected = jnp.dot(normed, in_weights[tower_index].reshape(D, 4 * HW), preferred_element_type=jnp.float32)
    positions = (offsets[tower_index, 0] + jnp.arange(TOK, dtype=jnp.int32)).astype(jnp.float32)
    head_gains = qk_gains[tower_index].reshape(3, HEADS, HD)
    finished = finish(projected.reshape(TOK, 4, HEADS, HD), head_gains, positions)
    return (states, modulate, finished.astype(jnp.bfloat16))

def heads_attend(queries, key_rows, value_rows, key_count):
    stacked = (jnp.swapaxes(queries, 0, 1), jnp.swapaxes(key_rows, 0, 1), jnp.swapaxes(value_rows, 0, 1))
    result = lax.map(lambda triple: attend(triple[0], triple[1], triple[2], key_count), stacked)
    return jnp.swapaxes(result, 0, 1).reshape(queries.shape[0], HW)

def branch_sum(self_out, cross_out, weights):
    block_width = HW // N_TP

    def accumulate(total_sum, block_index):
        row_start = block_index * block_width
        self_part = lax.dynamic_slice_in_dim(self_out, row_start, block_width, 1)
        cross_part = lax.dynamic_slice_in_dim(cross_out, row_start, block_width, 1)
        self_weight = lax.dynamic_slice_in_dim(weights[0], row_start, block_width, 0)
        cross_weight = lax.dynamic_slice_in_dim(weights[1], row_start, block_width, 0)
        partial_term = jnp.dot(self_part, self_weight, preferred_element_type=jnp.float32) + jnp.dot(cross_part, cross_weight, preferred_element_type=jnp.float32)
        rounded = lax.optimization_barrier(partial_term.astype(jnp.bfloat16))
        return (total_sum + rounded.astype(jnp.float32), None)
    total_sum, unused = lax.scan(accumulate, jnp.zeros((TOK, D), jnp.float32), jnp.arange(N_TP, dtype=jnp.int32))
    return total_sum

def reference(hidden, modulation, qk_gains, counts, offsets, in_weights, out_weights):
    prepared = [prepare(tower_index, hidden, modulation, qk_gains, offsets, in_weights) for tower_index in range(2)]
    outputs = []
    for tower_index in range(2):
        states, modulate, projected = prepared[tower_index]
        opposite = prepared[1 - tower_index][2]
        self_out = heads_attend(projected[:, 0], projected[:, 1], projected[:, 2], counts[tower_index, 0])
        cross_out = heads_attend(projected[:, 3], opposite[:, 1], opposite[:, 2], counts[1 - tower_index, 0])
        branch = branch_sum(self_out, cross_out, out_weights[tower_index])
        outputs.append((states + modulate[2] * branch).astype(jnp.bfloat16))
    return jnp.stack(outputs, 0)
```

```python
import functools
import math

import jax
import jax.numpy as jnp
import numpy as np
from jax import lax
from jax.experimental import pallas as pl
from jax.experimental.pallas import tpu as pltpu
from jax.sharding import PartitionSpec as P

EPS = 1e-6
ROPE_BASE = 10000.0
MASKED = -1e30
MESH = pl.DeviceIdType.MESH
F32 = jnp.float32
BF16 = jnp.bfloat16


def index_of(pos, n):
    upper = pos // (n // 2)
    return (1 - upper) * (2 * pos) + upper * (2 * (n - 1 - pos) + 1)


def position_of(index, n):
    odd = index % 2
    return (1 - odd) * (index // 2) + odd * (n - 1 - index // 2)


def kernel(
    n, counts_hbm, offsets_hbm, hidden_hbm, mod_hbm, gains_hbm, freq_hbm, w_hbm, wo_hbm, out_ref,
    counts_ref, offsets_ref, hidden_ref, mod_ref, gains_ref, freq_ref, w_raw, w, wo, xg, cos_t, sin_t, qc, kv, kv_other, both, part, from_left, from_right,
    in_sem, w_sem, wo_sem, ag_send, ag_recv, kv_send, kv_recv, rs_send, rs_recv,
):
    rows, width = hidden_hbm.shape
    pieces = 4
    fine = rows // pieces
    strip = width // pieces
    total = rows * n
    hd = freq_ref.shape[-1]
    reach = n // 2
    tower = lax.axis_index("tower")
    me = lax.axis_index("tp")
    pos = position_of(me, n)
    right = index_of((pos + 1) % n, n)
    left = index_of((pos + n - 1) % n, n)

    barrier = pltpu.get_barrier_semaphore()
    pl.semaphore_signal(barrier, inc=1, device_id={"tp": left}, device_id_type=MESH)
    pl.semaphore_signal(barrier, inc=1, device_id={"tp": right}, device_id_type=MESH)
    pl.semaphore_signal(barrier, inc=1, device_id={"tower": 1 - tower}, device_id_type=MESH)
    hidden_copy = pltpu.make_async_copy(hidden_hbm, hidden_ref, in_sem.at[0])
    hidden_copy.start()
    mod_copy = pltpu.make_async_copy(mod_hbm, mod_ref, in_sem.at[1])
    mod_copy.start()
    w_copy = pltpu.make_async_copy(w_hbm, w_raw, w_sem)
    w_copy.start()
    wo_copy = pltpu.make_async_copy(wo_hbm, wo, wo_sem)
    wo_copy.start()
    small_copies = [
        pltpu.make_async_copy(source, target, in_sem.at[2 + order])
        for order, (source, target) in enumerate((
            (offsets_hbm, offsets_ref), (counts_hbm, counts_ref), (freq_hbm, freq_ref), (gains_hbm, gains_ref),
        ))
    ]
    for copy in small_copies:
        copy.start()
    def at_distance(d):
        return index_of((pos + n + d) % n, n)

    def block(index):
        return pl.ds(pl.multiple_of(index * rows, rows), rows)

    def piece(index, h):
        return pl.ds(pl.multiple_of(index * rows + h * fine, fine), fine)

    def strip_of(h):
        return pl.ds(h * strip, strip)

    hidden_copy.wait()
    mod_copy.wait()
    states = hidden_ref[...].astype(F32)
    centre = states - jnp.mean(states, -1, keepdims=True)
    spread = jnp.mean(centre * centre, -1, keepdims=True)
    normed = centre * lax.rsqrt(spread + EPS) * (1.0 + mod_ref[1]) + mod_ref[0]
    xg[block(me), :] = normed.astype(BF16)
    pl.semaphore_wait(barrier, 3)

    def gather_copy(way, step, h, index):
        return pltpu.make_async_remote_copy(
            src_ref=xg.at[block(index), strip_of(h)],
            dst_ref=xg.at[block(index), strip_of(h)],
            send_sem=ag_send.at[way, step, h],
            recv_sem=ag_recv.at[way, step, h],
            device_id={"tp": left if way else right},
            device_id_type=MESH,
        )

    for turn in range(pieces):
        gather_copy(0, 0, turn, me).start()
        gather_copy(1, 0, pieces - 1 - turn, me).start()

    w_copy.wait()
    span = 256
    quarter = span // 4
    to_row = lax.broadcasted_iota(jnp.int32, (span, span), 0)
    from_row = lax.broadcasted_iota(jnp.int32, (span, span), 1)
    sorter = jnp.where(from_row == 4 * (to_row % quarter) + to_row // quarter, 1.0, 0.0).astype(BF16)

    def sort_rows(i, carry):
        tile = w_raw[pl.ds(pl.multiple_of(i * span, span), span), :]
        moved = jnp.dot(sorter, tile, preferred_element_type=F32).astype(BF16)
        to = pl.ds(pl.multiple_of(i * quarter, quarter), quarter)
        for c, place in enumerate((2, 0, 1, 3)):
            w[to, place * hd:(place + 1) * hd] = moved[c * quarter:(c + 1) * quarter]
        return carry

    lax.fori_loop(0, w_raw.shape[0] // span, sort_rows, 0, unroll=8)

    lane = lax.broadcasted_iota(jnp.int32, (1, hd), 1)
    even_lane = lane % 2 == 0

    def take(step, forward_both):
        from_l, from_r = at_distance(-step), at_distance(step)
        for turn in range(pieces):
            for way, h, index in ((0, turn, from_l), (1, pieces - 1 - turn, from_r)):
                gather_copy(way, step - 1, h, index).wait_recv()
                if turn < pieces // 2:
                    gather_copy(way, step, h, index).start()
                else:
                    @pl.when(forward_both)
                    def _():
                        gather_copy(way, step, h, index).start()

    def kv_copy(index, slot):
        return pltpu.make_async_remote_copy(
            src_ref=kv.at[block(index), :],
            dst_ref=kv_other.at[block(index), :],
            send_sem=kv_send.at[slot],
            recv_sem=kv_recv.at[slot],
            device_id={"tower": 1 - tower},
            device_id_type=MESH,
        )

    def project(indices, slots, parts=None):
        cosine = jnp.concatenate([cos_t[block(i), :] for i in indices], 0)
        sine = jnp.concatenate([sin_t[block(i), :] for i in indices], 0)

        def finish(value, gain):
            squares = jnp.mean(value * value, -1, keepdims=True)
            value = value * lax.rsqrt(squares + EPS) * gains_ref[gain]
            swapped = jnp.where(
                even_lane, pltpu.roll(value, hd - 1, 1), pltpu.roll(value, 1, 1)
            )
            return (value * cosine + swapped * sine).astype(BF16)

        def put(to, column, value):
            for order, i in enumerate(indices):
                to[block(i), column:column + hd] = value[order * rows:(order + 1) * rows]

        def product(columns):
            if parts is None:
                x = jnp.concatenate([xg[block(i), :] for i in indices], 0)
                return jnp.dot(x, w[:, columns], preferred_element_type=F32)
            early, late = parts
            done = early[:, columns]
            for first, end in late:
                x = jnp.concatenate([xg[block(i), first:end] for i in indices], 0)
                done = done + jnp.dot(x, w[first:end, columns], preferred_element_type=F32)
            return done

        if parts is not None:
            projected = product(slice(0, 4 * hd))
            key, query, cross = (
                finish(projected[:, c * hd:(c + 1) * hd], gain) for c, gain in ((0, 1), (2, 0), (3, 2))
            )
            put(kv, 0, key)
            put(kv, hd, projected[:, hd:2 * hd].astype(BF16))
            put(qc, 0, query)
            put(qc, hd, cross)
            for i, slot in zip(indices, slots):
                kv_copy(i, slot).start()
            return
        projected = product(slice(0, 2 * hd))
        put(kv, 0, finish(projected[:, 0:hd], 1))
        put(kv, hd, projected[:, hd:2 * hd].astype(BF16))
        for i, slot in zip(indices, slots):
            kv_copy(i, slot).start()
        projected = product(slice(2 * hd, 4 * hd))
        put(qc, 0, finish(projected[:, 0:hd], 0))
        put(qc, hd, finish(projected[:, hd:2 * hd], 2))

    take(1, reach > 2)
    for copy in small_copies:
        copy.wait()
    own_offset = offsets_ref[tower]
    chunk = min(256, total)
    for first in range(0, total, chunk):
        row = lax.broadcasted_iota(jnp.int32, (chunk, hd), 0) + (own_offset + first)
        angles = row.astype(F32) * freq_ref[...]
        cos_t[first:first + chunk, :] = jnp.cos(angles)
        sine = jnp.sin(angles)
        sin_t[first:first + chunk, :] = jnp.where(even_lane, -sine, sine)
    project([me, at_distance(-1), at_distance(1)], [0, 1, 2])

    def gather_step(step, carry):
        take(step, step < reach - 1)
        project([at_distance(-step), at_distance(step)], [2 * step - 1, 2 * step])
        return carry

    lax.fori_loop(2, reach, gather_step, 0)
    far = at_distance(reach)
    middle = pieces // 2 - 1
    early = jnp.zeros((rows, 4 * hd), F32)
    for turn in range(pieces // 2):
        gather_copy(0, reach - 1, turn, far).wait_recv()
        gather_copy(1, reach - 1, pieces - 1 - turn, far).wait_recv()
        if turn < middle:
            for h in (turn, pieces - 1 - turn):
                held = slice(h * strip, (h + 1) * strip)
                early = early + jnp.dot(xg[block(far), held], w[held, :], preferred_element_type=F32)
    project([far], [n - 1], (early, [(middle * strip, (pieces - middle) * strip)]))

    key_index = lax.broadcasted_iota(jnp.int32, (1, total), 1)

    def attend(indices):
        sides = ((kv, 0, counts_ref[tower]), (kv_other, hd, counts_ref[1 - tower]))
        query = jnp.concatenate([qc[block(i), :] for i in indices], 0)
        scores = [
            lax.dot_general(
                query[:, column:column + hd], source[:, 0:hd], (((1,), (1,)), ((), ())), preferred_element_type=F32
            ) * (1.0 / math.sqrt(hd))
            for source, column, _ in sides
        ]
        scores = [jnp.where(key_index < count, s, MASKED) for s, (_, _, count) in zip(scores, sides)]
        raised = [jnp.exp(s - jnp.max(s, -1, keepdims=True)) for s in scores]
        weights = [(r * (1.0 / jnp.sum(r, -1, keepdims=True))).astype(BF16) for r in raised]
        results = [
            jnp.dot(weight, source[:, hd:2 * hd], preferred_element_type=F32).astype(BF16)
            for weight, (source, _, _) in zip(weights, sides)
        ]
        result = jnp.concatenate(results, 1)
        for order, i in enumerate(indices):
            both[block(i), :] = result[order * rows:(order + 1) * rows]

    up, down = at_distance(reach - 1), at_distance(1 - reach)
    wo_copy.wait()
    for slot in range(n):
        kv_copy(me, slot).wait_recv()
    attend([far])

    def partial_terms(indices, order, ready=None):
        x = jnp.concatenate([both[block(i), :] for i in indices], 0)
        for h in order:
            term = jnp.dot(x, wo[:, h * strip:(h + 1) * strip], preferred_element_type=F32).astype(BF16)
            for place, i in enumerate(indices):
                part[block(i), h * strip:(h + 1) * strip] = term[place * rows:(place + 1) * rows]
            if ready is not None:
                ready(h)

    def scatter_copy(way, slot, h, source):
        slots = from_right if way else from_left
        return pltpu.make_async_remote_copy(
            src_ref=source,
            dst_ref=slots.at[slot, h],
            send_sem=rs_send.at[way, slot, h],
            recv_sem=rs_recv.at[way, slot, h],
            device_id={"tp": left if way else right},
            device_id_type=MESH,
        )

    def part_strip(index, h):
        return part.at[block(index), strip_of(h)]

    inward = [h for pair in zip(range(pieces // 2), range(pieces - 1, pieces // 2 - 1, -1)) for h in pair]

    def send_far(h):
        scatter_copy(int(h >= pieces // 2), 0, h, part_strip(far, h)).start()

    partial_terms([far], inward, send_far)

    def pass_on(way, slot, h, index):
        slots = from_right if way else from_left
        held = slots.at[slot, h]
        scatter_copy(way, slot, h, held).wait_recv()
        slots[slot, h] = (
            slots[slot, h].astype(F32) + part[block(index), strip_of(h)].astype(F32)
        ).astype(BF16)
        scatter_copy(way, slot + 1, h, held).start()

    def send_near(h):
        way = int(h < pieces // 2)
        scatter_copy(way, 1, h, part_strip(down if way else up, h)).start()

    attend([up, down])
    partial_terms([up, down], inward[::-1], send_near)
    def gathered(step, carry):
        for way in range(2):
            for h in range(pieces):

                @pl.when((step < reach - 1) | ((h // (pieces // 2)) == way))
                def _():
                    gather_copy(way, step, h, me).wait_send()
        return carry

    for slot in range(n):
        kv_copy(me, slot).wait_send()
    lax.fori_loop(0, reach, gathered, 0)
    for turn in range(pieces // 2):
        pass_on(0, 0, turn, up)
        pass_on(1, 0, pieces - 1 - turn, down)

    short_first = (*range(pieces // 2, pieces), *range(pieces // 2))

    def scatter_step(slot, carry):
        up, down = at_distance(reach - 1 - slot), at_distance(1 + slot - reach)
        attend([up, down])
        partial_terms([up, down], range(pieces))
        for turn in short_first:
            pass_on(0, slot, turn, up)
            pass_on(1, slot, pieces - 1 - turn, down)
        return carry

    lax.fori_loop(1, reach - 1, scatter_step, 0)
    attend([me])
    partial_terms([me], range(pieces))
    last = reach - 1
    gate = mod_ref[2]

    def scattered(step, carry):
        for way in range(2):
            for h in range(pieces):

                @pl.when((step > 0) | ((h // (pieces // 2)) == way))
                def _():
                    scatter_copy(way, step, h, from_left.at[0, h]).wait_send()
        return carry

    lax.fori_loop(0, last, scattered, 0)
    for h in range(pieces):
        scatter_copy(0, last, h, from_left.at[last, h]).wait_recv()
        scatter_copy(1, last, h, from_right.at[last, h]).wait_recv()
    for h in range(pieces):
        columns = slice(h * strip, (h + 1) * strip)
        branch = (
            part[block(me), columns].astype(F32)
            + from_left[last, h].astype(F32)
            + from_right[last, h].astype(F32)
        )
        held = hidden_ref[:, columns].astype(F32)
        out_ref[:, columns] = (held + gate[:, columns] * branch).astype(BF16)
    for way in range(2):
        for h in range(pieces):
            scatter_copy(way, last, h, from_left.at[0, h]).wait_send()


def local(n, hidden, modulation, qk_gains, counts, offsets, in_weights, out_weights):
    _, rows, width = hidden.shape
    hd = in_weights.shape[-1]
    total, pieces, reach = rows * n, 4, n // 2
    pairs = np.arange(hd) // 2
    freq = np.power(ROPE_BASE, -2.0 * pairs / hd).astype(np.float32)[None]
    vmem = pl.BlockSpec(memory_space=pltpu.VMEM)
    hbm = pl.BlockSpec(memory_space=pltpu.HBM)
    buffers = [
        pltpu.SMEM((2,), jnp.int32),
        pltpu.SMEM((2,), jnp.int32),
        pltpu.VMEM((rows, width), BF16),
        pltpu.VMEM((3, 1, width), F32),
        pltpu.VMEM((3, 1, hd), F32),
        pltpu.VMEM((1, hd), F32),
        pltpu.VMEM((4 * width, hd), BF16),
        pltpu.VMEM((width, 4 * hd), BF16),
        pltpu.VMEM((2 * hd, width), BF16),
        pltpu.VMEM((total, width), BF16),
        pltpu.VMEM((total, hd), F32),
        pltpu.VMEM((total, hd), F32),
        pltpu.VMEM((total, 2 * hd), BF16),
        pltpu.VMEM((total, 2 * hd), BF16),
        pltpu.VMEM((total, 2 * hd), BF16),
        pltpu.VMEM((total, 2 * hd), BF16),
        pltpu.VMEM((total, width), BF16),
        pltpu.VMEM((reach, pieces, rows, width // pieces), BF16),
        pltpu.VMEM((reach, pieces, rows, width // pieces), BF16),
    ]
    out = pl.pallas_call(
        functools.partial(kernel, n),
        out_shape=pltpu.VMEM((rows, width), BF16),
        in_specs=[hbm] * 8,
        out_specs=vmem,
        scratch_shapes=[
            *buffers,
            pltpu.SemaphoreType.DMA((6,)),
            pltpu.SemaphoreType.DMA,
            pltpu.SemaphoreType.DMA,
            pltpu.SemaphoreType.DMA((2, reach, pieces)),
            pltpu.SemaphoreType.DMA((2, reach, pieces)),
            pltpu.SemaphoreType.DMA((n,)),
            pltpu.SemaphoreType.DMA((n,)),
            pltpu.SemaphoreType.DMA((2, reach, pieces)),
            pltpu.SemaphoreType.DMA((2, reach, pieces)),
        ],
        compiler_params=pltpu.CompilerParams(
            collective_id=0, has_side_effects=True, vmem_limit_bytes=60 * 1024 * 1024
        ),
    )(
        counts[:, 0],
        offsets[:, 0],
        hidden[0],
        modulation.reshape(3, 1, width),
        qk_gains.reshape(3, 1, hd),
        jnp.asarray(freq),
        in_weights.reshape(4 * width, hd),
        out_weights.reshape(2 * hd, width),
    )
    return out[None]


def solution(mesh):
    return jax.shard_map(
        functools.partial(local, mesh.shape["tp"]),
        mesh=mesh,
        in_specs=(
            P("tower", ("grp", "tp"), None),
            P("tower", None, None),
            P("tower", None, "tp"),
            P(None, "grp"),
            P(None, "grp"),
            P("tower", None, None, "tp"),
            P("tower", None, "tp", None),
        ),
        out_specs=P("tower", ("grp", "tp"), None),
        check_vma=False,
    )
```
